32 devices in a mesh: gx: 4 (over y, x), gy: 8 (over z, core).
Axes of the slice: x: 2, y: 2, z: 4, core: 2. Of those that a mesh axis runs over, the one named last changes fastest.
Arguments:
- u_wind: float32 [64, 64, 1024], P(None, 'gx', 'gy'), may hold values from -6 to 6
- v_wind: float32 [64, 64, 1024], P(None, 'gx', 'gy'), may hold values from -6 to 6
- w_wind: float32 [64, 64, 1024], P(None, 'gx', 'gy'), may hold values from -4 to 4
- pressure: float32 [64, 64, 1024], P(None, 'gx', 'gy'), may hold values from -6 to 6
- terrain_level: int32 [64, 1024], P('gx', 'gy'), may hold values from 0 to 8
- zone_width: int32 [4], replicated, may hold values from 5 to 16
- stiffness: float32 [64], replicated, may hold values from 0.25 to 2
- inflow_profile: float32 [2, 64], replicated, may hold values from -5 to 5
Outputs:
- u_final: float32 [64, 64, 1024], P(None, 'gx', 'gy')
- v_final: float32 [64, 64, 1024], P(None, 'gx', 'gy')
- w_final: float32 [64, 64, 1024], P(None, 'gx', 'gy')
- p_final: float32 [64, 64, 1024], P(None, 'gx', 'gy')
The draws below stay inside these ranges and needn't reach their ends.
Inputs may be any that keep to these rules, and one draw needn't show every extreme that they name: `zone_width`: zone widths in columns.
All inputs are finite; a program needn't handle non-finite values.
Results may differ from the reference program's by a relative error of at most 0.0001.
Values sent between devices are 32-bit elements; how exact they have to be, the bound alone decides.
A program may use at most 128 MiB of HBM per device.

```python
import math
import jax
import jax.numpy as jnp
from jax import lax

NZ = 64
SUB = 6
TERRAIN_MAX = 8
ZONE_MAX = 16
NX = 64
NY = 1024


def place_ends(values, rng, least, largest):
    dims = values.shape
    index_at = [jax.random.randint(jax.random.fold_in(rng, axis), (), 0, dims[axis]) for axis in range(len(dims))]
    values = values.at[tuple(index_at)].set(least)
    longest = dims.index(max(dims))
    index_at[longest] = (index_at[longest] + 1) % dims[longest]
    return values.at[tuple(index_at)].set(largest)


def block_scale(key, shape, split, smallest, high):
    gain = 1.0
    for dim, shards_of in split:
        heights = jax.random.uniform(jax.random.fold_in(jax.random.fold_in(key, 6), dim), (shards_of,), jnp.float32, smallest / len(split), high / len(split))
        gain = gain * jnp.repeat(jnp.exp(heights), shape[dim] // shards_of).reshape((-1,) + (1,) * (len(shape) - 1 - dim))
    return gain


def centred(rng, shape, spread, most, split=(), held_as=jnp.bfloat16):
    drawn = jax.random.normal(rng, shape, jnp.float32) * spread
    if len(split) > 0:
        drawn = block_scale(rng, shape, split, -0.22, 0.18) * drawn
    return jnp.clip(drawn, min=-most, max=most).astype(held_as)


def setup_inputs(seed: int = 0) -> dict:
    seeds = jax.random.split(jax.random.key(seed), 9)
    u_wind = centred(seeds[0], (NZ, NX, NY), 1.0, 6.0, ((1, 4), (2, 8)), jnp.float32)
    v_wind = centred(seeds[1], (NZ, NX, NY), 1.0, 6.0, ((1, 4), (2, 8)), jnp.float32)
    w_wind = centred(seeds[2], (NZ, NX, NY), 0.5, 4.0, ((1, 4), (2, 8)), jnp.float32)
    pressure = centred(seeds[3], (NZ, NX, NY), 1.0, 6.0, ((1, 4), (2, 8)), jnp.float32)
    terrain_level = place_ends(jax.random.randint(seeds[4], (NX, NY), 0, TERRAIN_MAX + 1), jax.random.fold_in(seeds[4], 1), 0, TERRAIN_MAX).astype(jnp.int32)
    zone_width = place_ends(jax.random.randint(seeds[5], (4,), ZONE_MAX // 4 + 1, ZONE_MAX + 1), jax.random.fold_in(seeds[5], 1), ZONE_MAX // 4 + 1, ZONE_MAX).astype(jnp.int32)
    stiffness = jnp.clip(jnp.exp(jax.random.uniform(seeds[6], (NZ,), jnp.float32, math.log(0.25), math.log(2.0))), 0.25, 2.0)
    inflow_profile = centred(seeds[7], (2, NZ), 1.0, 5.0, (), jnp.float32)
    return dict(u_wind=u_wind, v_wind=v_wind, w_wind=w_wind, pressure=pressure, terrain_level=terrain_level, zone_width=zone_width, stiffness=stiffness, inflow_profile=inflow_profile)


ADV_COURANT = 0.3
H_COURANT = 0.4
Z_COURANT = 1.0
RELAX_STRENGTH = 0.5


def face_flux(scalar, velocity, along):
    extent = scalar.shape[along]
    count = extent - 5

    def offset(start):
        return lax.slice_in_dim(scalar, start, start + count, axis=along)

    centered = (37.0 * (offset(3) + offset(2)) - 8.0 * (offset(4) + offset(1)) + (offset(5) + offset(0))) / 60.0
    upwind = (10.0 * (offset(3) - offset(2)) - 5.0 * (offset(4) - offset(1)) + (offset(5) - offset(0))) / 60.0
    face_speed = lax.slice_in_dim(velocity, 3, 3 + count, axis=along)
    flux = face_speed * centered - jnp.abs(face_speed) * upwind
    return lax.slice_in_dim(flux, 1, count, axis=along) - lax.slice_in_dim(flux, 0, count - 1, axis=along)


def advect(extended, wet_inner):
    west_east = extended[0]
    south_north = extended[1]
    first = west_east.shape[1]
    second = west_east.shape[2]
    results = []
    for scalar in extended:
        tend_x = face_flux(scalar, west_east, 1)[:, :, 3:second - 3]
        tend_y = face_flux(scalar, south_north, 2)[:, 3:first - 3, :]
        inner = scalar[:, 3:first - 3, 3:second - 3]
        results.append(wet_inner * (inner - ADV_COURANT * (tend_x + tend_y)))
    return results


def relax_plane(col_index, row_index, x_total, y_total, zones):
    zone_f = zones.astype(jnp.float32)
    west_ramp = jnp.maximum(zone_f[0] - col_index, 0.0) / zone_f[0]
    east_ramp = jnp.maximum(zone_f[1] - (x_total - 1.0 - col_index), 0.0) / zone_f[1]
    south_ramp = jnp.maximum(zone_f[2] - row_index, 0.0) / zone_f[2]
    north_ramp = jnp.maximum(zone_f[3] - (y_total - 1.0 - row_index), 0.0) / zone_f[3]
    along_x = jnp.maximum(west_ramp, east_ramp)[:, None]
    along_y = jnp.maximum(south_ramp, north_ramp)[None, :]
    return RELAX_STRENGTH * jnp.maximum(along_x, along_y)


def thomas(sub_diag, main_diag, super_diag, right_side):
    def eliminate(carry, row):
        c_prev, d_prev = carry
        low_row, main_row, up_row, rhs_row = row
        pivot_value = main_row - low_row * c_prev
        c_new = up_row / pivot_value
        d_new = (rhs_row - low_row * d_prev) / pivot_value
        return (c_new, d_new), (c_new, d_new)

    zero_plane = jnp.zeros_like(main_diag[0])
    unused, (c_all, d_all) = lax.scan(eliminate, (zero_plane, zero_plane), (sub_diag, main_diag, super_diag, right_side), unroll=8)

    def substitute(x_next, row):
        c_row, d_row = row
        value = d_row - c_row * x_next
        return value, value

    unused_last, solved = lax.scan(substitute, zero_plane, (c_all, d_all), reverse=True, unroll=8)
    return solved


def shift_down(field):
    return jnp.concatenate([jnp.zeros_like(field[:1]), field[:-1]], axis=0)


def shift_up(field):
    return jnp.concatenate([field[1:], jnp.zeros_like(field[:1])], axis=0)


def column_solve(w_wind, q_field, wet_mask, g_level):
    factor = Z_COURANT * Z_COURANT
    g_cell = g_level * wet_mask
    g_above = shift_up(g_cell)
    wet_below = shift_down(wet_mask)
    sub_diag = -factor * g_cell * wet_below
    super_diag = -factor * g_above * wet_mask
    main_diag = 1.0 + wet_mask * factor * (g_above + g_cell)
    right_side = wet_mask * (w_wind - Z_COURANT * (shift_up(q_field) - q_field))
    return thomas(sub_diag, main_diag, super_diag, right_side)


def local_west(field):
    return jnp.concatenate([jnp.zeros_like(field[:, :1, :]), field[:, :-1, :]], axis=1)


def local_east(field):
    return jnp.concatenate([field[:, 1:, :], jnp.zeros_like(field[:, :1, :])], axis=1)


def local_south(field):
    return jnp.concatenate([jnp.zeros_like(field[:, :, :1]), field[:, :, :-1]], axis=2)


def local_north(field):
    return jnp.concatenate([field[:, :, 1:], jnp.zeros_like(field[:, :, :1])], axis=2)


def substep_update(carried, wet_mask, relax, g_level, u_bound, v_bound, from_west, from_south, from_east, from_north):
    u_wind, v_wind, w_wind, pressure = carried
    u_wind = wet_mask * (u_wind - H_COURANT * (pressure - from_west(pressure)))
    v_wind = wet_mask * (v_wind - H_COURANT * (pressure - from_south(pressure)))
    divergence = H_COURANT * (from_east(u_wind) - u_wind + from_north(v_wind) - v_wind)
    q_field = wet_mask * (pressure - g_level * divergence)
    w_wind = column_solve(w_wind, q_field, wet_mask, g_level)
    pressure = wet_mask * (q_field - g_level * Z_COURANT * (w_wind - shift_down(w_wind)))
    u_wind = u_wind - relax * (u_wind - wet_mask * u_bound)
    v_wind = v_wind - relax * (v_wind - wet_mask * v_bound)
    w_wind = w_wind - relax * w_wind
    pressure = pressure - relax * pressure
    return (u_wind, v_wind, w_wind, pressure)


def reference(u_wind, v_wind, w_wind, pressure, terrain_level, zone_width, stiffness, inflow_profile):
    levels = jnp.arange(NZ).astype(jnp.float32)[:, None, None]
    wet_mask = (levels >= terrain_level.astype(jnp.float32)[None, :, :]).astype(jnp.float32)
    padding = ((0, 0), (3, 3), (3, 3))
    extended = [jnp.pad(field, padding) for field in (u_wind, v_wind, w_wind, pressure)]
    carried = tuple(advect(extended, wet_mask))
    col_index = jnp.arange(NX).astype(jnp.float32)
    row_index = jnp.arange(NY).astype(jnp.float32)
    relax = relax_plane(col_index, row_index, float(NX), float(NY), zone_width)
    g_level = stiffness[:, None, None]
    u_bound = inflow_profile[0][:, None, None]
    v_bound = inflow_profile[1][:, None, None]
    for substep in range(SUB):
        carried = substep_update(carried, wet_mask, relax, g_level, u_bound, v_bound, local_west, local_south, local_east, local_north)
    return carried[0], carried[1], carried[2], carried[3]
```

```python
import functools

import jax
import jax.numpy as jnp
from jax import lax
from jax.experimental import pallas as pl
from jax.experimental.pallas import tpu as pltpu
from jax.sharding import PartitionSpec as P

SUB = 6
ADV = 0.3
HC = 0.4
ZC = 1.0
RELAX = 0.5
EXT = 32
LO = 8
DRY = 1 << 20
WEST, EAST, SOUTH, NORTH = 0, 1, 2, 3
CHUNK = 4


def stencil(c, m3, m2, m1, f0, e1, e2):
    centered = 37.0 * (f0 + m1) - 8.0 * (e1 + m2) + (e2 + m3)
    upwind = 10.0 * (f0 - m1) - 5.0 * (e1 - m2) + (e2 - m3)
    return c * centered - jnp.abs(c) * upwind


def kernel(
    nz,
    bx,
    cnt,
    u_in,
    v_in,
    w_in,
    p_in,
    terr,
    zone,
    g,
    prof,
    u_out,
    v_out,
    w_out,
    p_out,
    u_ext,
    v_ext,
    w_ext,
    p_ext,
    tend,
    q_buf,
    d_buf,
    w_buf,
    cc,
    li,
    wi,
    xs,
    xr,
    ys,
    yr,
    g_lo,
    g_hi,
    trx,
    tr_y,
    terr_ext,
    ps_x,
    pr_x,
    ps_y,
    pr_y,
    us_x,
    ur_x,
    vs_y,
    vr_y,
    ub_x,
    wet_x,
    uh_x,
    ini_s,
    ini_r,
    ter_s,
    ter_r,
    uv_s,
    uv_r,
    stp_s,
    stp_r,
):
    by = 128
    gx = lax.axis_index("gx")
    gy = lax.axis_index("gy")
    nx_dev, ny_dev = cnt
    has = (gx > 0, gx < nx_dev - 1, gy > 0, gy < ny_dev - 1)
    peer = ({"gx": gx - 1}, {"gx": gx + 1}, {"gy": gy - 1}, {"gy": gy + 1})
    opp = (EAST, WEST, NORTH, SOUTH)
    exts = (u_ext, v_ext, w_ext, p_ext)
    ins = (u_in, v_in, w_in, p_in)

    barrier = pltpu.get_barrier_semaphore()
    for d in range(4):

        @pl.when(has[d])
        def _(d=d):
            pl.semaphore_signal(
                barrier, inc=1, device_id=peer[d], device_id_type=pl.DeviceIdType.MESH
            )

    def rcopy(d, src, dst, ss, rs):
        return pltpu.make_async_remote_copy(
            src_ref=src,
            dst_ref=dst,
            send_sem=ss,
            recv_sem=rs,
            device_id=peer[d],
            device_id_type=pl.DeviceIdType.MESH,
        )

    def start(d, *args):
        @pl.when(has[d])
        def _():
            rcopy(d, *args).start()

    def wait_send(d, *args):
        @pl.when(has[d])
        def _():
            rcopy(d, *args).wait_send()

    def wait_recv(d, *args):
        @pl.when(has[opp[d]])
        def _():
            rcopy(d, *args).wait_recv()

    def ini(d, f):
        if d < 2:
            return xs.at[d, f], xr.at[d, f], ini_s.at[d, f], ini_r.at[d, f]
        return ys.at[d - 2, f], yr.at[d - 2, f], ini_s.at[d, f], ini_r.at[d, f]

    def ter(d):
        if d == WEST:
            return terr.at[pl.ds(0, 8)], trx, ter_s.at[0], ter_r.at[0]
        return terr, tr_y, ter_s.at[1], ter_r.at[1]

    def uv(d):
        if d == WEST:
            return us_x, ur_x, uv_s.at[0], uv_r.at[0]
        return vs_y, vr_y, uv_s.at[1], uv_r.at[1]

    def stp(d, s):
        if d < 2:
            return ps_x.at[d, s], pr_x.at[d, s], stp_s.at[d, s], stp_r.at[d, s]
        return ps_y.at[s], pr_y.at[d - 2, s], stp_s.at[d, s], stp_r.at[d, s]

    rows = lax.broadcasted_iota(jnp.int32, (bx, by), 0)
    lane = lax.broadcasted_iota(jnp.int32, (bx, by), 1)

    def slab(k):
        return pl.ds(pl.multiple_of(k * bx, bx), bx)

    def ext_at(k, off, n):
        return pl.ds(k * EXT + off, n)

    def own(k):
        return pl.ds(pl.multiple_of(k * EXT + LO, 8), bx)

    def edge(ref, off):
        return [ref[pl.ds(k * EXT + off, 8, stride=EXT), :] for k in range(0, nz, 8)]

    for d in range(4):

        @pl.when(jnp.logical_not(has[opp[d]]))
        def _(d=d):
            if d < 2:
                xr[d] = jnp.zeros(xr.shape[1:], jnp.float32)
                pr_x[d] = jnp.zeros(pr_x.shape[1:], jnp.float32)
            else:
                yr[d - 2] = jnp.zeros(yr.shape[1:], jnp.float32)
                pr_y[d - 2] = jnp.zeros(pr_y.shape[1:], jnp.float32)
            if d == WEST:
                trx[...] = jnp.full(trx.shape, DRY, jnp.int32)
                ur_x[...] = jnp.zeros(ur_x.shape, jnp.float32)
            if d == SOUTH:
                tr_y[...] = jnp.full(tr_y.shape, DRY, jnp.int32)
                vr_y[...] = jnp.zeros(vr_y.shape, jnp.float32)

    neighbours = sum(h.astype(jnp.int32) for h in has)
    pl.semaphore_wait(barrier, neighbours)
    start(WEST, *ter(WEST))
    start(SOUTH, *ter(SOUTH))

    for f in range(4):
        for r in range(3):
            for k in range(0, nz, 8):
                xs[WEST, f, pl.ds(r * nz + k, 8), :] = ins[f][pl.ds(k * bx + r, 8, stride=bx), :]
                xs[EAST, f, pl.ds(r * nz + k, 8), :] = ins[f][
                    pl.ds(k * bx + bx - 3 + r, 8, stride=bx), :
                ]
        start(WEST, *ini(WEST, f))
        start(EAST, *ini(EAST, f))

    group = by // 8
    for f in range(4):

        def pack(kg, carry, f=f):
            lo = hi = jnp.zeros((bx, by), jnp.float32)
            for kk in range(group):
                k = kg * group + kk
                x = ins[f][slab(k), :]
                exts[f][own(k), :] = x
                pick = (lane >> 3) == kk
                lo = jnp.where(pick, pltpu.roll(x, 8 * kk + 3, 1), lo)
                hi = jnp.where(pick, pltpu.roll(x, 8 * kk + 5, 1), hi)
            ys[SOUTH - 2, f, slab(kg), :] = lo
            ys[NORTH - 2, f, slab(kg), :] = hi
            return carry

        lax.fori_loop(0, nz // group, pack, 0)
        start(SOUTH, *ini(SOUTH, f))
        start(NORTH, *ini(NORTH, f))

    def relax_of(ci, rj):
        best = None
        for n, dist in enumerate(
            (
                ci,
                (nx_dev * bx - 1.0) - ci,
                rj,
                (ny_dev * by - 1.0) - rj,
            )
        ):
            width = jnp.full(ci.shape, zone[n], jnp.int32).astype(jnp.float32)
            ramp = jnp.maximum(width - dist, 0.0) / width
            best = ramp if best is None else jnp.maximum(best, ramp)
        return RELAX * best

    start_x = gx * bx
    start_y = gy * by
    ci = (rows + start_x).astype(jnp.float32)
    rj = (lane + start_y).astype(jnp.float32)
    relax = relax_of(ci, rj)
    keep = 1.0 - relax
    relax_hx = relax_of(
        (jnp.zeros((8, by), jnp.int32) + (start_x + bx)).astype(jnp.float32), rj[:8]
    )
    relax_hy = relax_of(ci, (jnp.zeros((bx, by), jnp.int32) + (start_y + by)).astype(jnp.float32))

    zero = jnp.zeros((bx, by), jnp.float32)
    for ref in (cc, li, wi, d_buf, w_buf):
        ref[pl.ds(0, bx), :] = zero
    t0 = terr[...]

    def coeff(k, carry):
        c_prev, vrow = carry
        above = jnp.minimum(k + 1, nz - 1)
        wet = jnp.where(t0 <= k, 1.0, 0.0)
        wet_b = jnp.where(jnp.logical_and(t0 <= k - 1, rows + k > rows), 1.0, 0.0)
        wet_a = jnp.where(jnp.logical_and(t0 <= k + 1, rows + (k + 1) < rows + nz), 1.0, 0.0)
        gk = (ZC * ZC) * g[k] * wet
        ga = (ZC * ZC) * g[above] * wet_a
        low = -gk * wet_b
        up = -ga * wet
        inv = 1.0 / (1.0 + wet * (ga + gk) - low * c_prev)
        c_new = up * inv
        cc[slab(k + 1), :] = c_new
        li[slab(k + 1), :] = low * inv
        wi[slab(k + 1), :] = wet * inv
        ub_x[pl.ds(k, 1), :] = jnp.full((1, by), prof[0, k], jnp.float32)
        vrow = jnp.where((lane >> 1) == k, prof[1, k], vrow)
        return c_new, vrow

    _, vb_y = lax.fori_loop(0, nz, coeff, (zero, zero))

    wait_recv(WEST, *ter(WEST))
    wait_recv(SOUTH, *ter(SOUTH))
    terr_ext[pl.ds(0, bx), :] = t0
    terr_ext[pl.ds(bx, 8), :] = trx[...]
    t1 = terr_ext[pl.ds(1, bx), :]
    t_east = jnp.broadcast_to(trx[0:1, :], (8, by))
    sub8 = lax.broadcasted_iota(jnp.int32, (8, by), 0)
    for k in range(0, nz, 8):
        wet_x[pl.ds(k, 8), :] = jnp.where(t_east <= sub8 + k, 1.0, 0.0)
    t_north = jnp.broadcast_to(tr_y[:, 0:1], (bx, by))
    wet_y = jnp.where(t_north <= (lane >> 1), 1.0, 0.0)

    scale = ADV / 60.0
    for f in range(4):
        wait_recv(SOUTH, *ini(SOUTH, f))
        wait_recv(NORTH, *ini(NORTH, f))

    def shifts(xw, xe):
        return (
            pltpu.roll(xw, 3, 1),
            pltpu.roll(xw, 2, 1),
            pltpu.roll(xw, 1, 1),
            xw,
            pltpu.roll(xe, by - 1, 1),
            pltpu.roll(xe, by - 2, 1),
        )

    def merge(kg, carry):
        at = slab(kg)

        def low(f):
            return jnp.where(
                (lane & 7) < 3,
                pltpu.roll(yr[NORTH - 2, f, at, :], by - 2, 1),
                ys[SOUTH - 2, f, at, :],
            )

        def high(f):
            return jnp.where(
                (lane & 7) < 5, ys[NORTH - 2, f, at, :], pltpu.roll(yr[SOUTH - 2, f, at, :], 2, 1)
            )

        c_lo = low(1) * scale
        c_hi = high(1) * scale
        for f in range(4):
            x = low(f)
            g_lo[f, at, :] = stencil(c_lo, *shifts(x, x))
            x = high(f)
            g_hi[f, at, :] = stencil(c_hi, *shifts(x, x))
        return carry

    lax.fori_loop(0, nz // group, merge, 0)

    def advect_y(k, carry):
        kg = k // group
        kk = k - kg * group
        c = v_ext[own(k), :] * scale
        for f in range(4):
            x = exts[f][own(k), :]
            lo = pltpu.roll(g_lo[f, slab(kg), :], by - 3 - 8 * kk, 1)
            hi = pltpu.roll(g_hi[f, slab(kg), :], by - 5 - 8 * kk, 1)
            flux = stencil(c, *shifts(x, x))
            flux = jnp.where(lane >= by - 2, hi, jnp.where(lane < 3, lo, flux))
            nxt = pltpu.roll(jnp.where(lane == 0, hi, flux), by - 1, 1)
            tend[f, slab(k), :] = x - (nxt - flux)
        return carry

    lax.fori_loop(0, nz, advect_y, 0, unroll=2)

    for f in range(4):
        wait_recv(WEST, *ini(WEST, f))
        wait_recv(EAST, *ini(EAST, f))
        for r in range(3):
            for k in range(0, nz, 8):
                exts[f][pl.ds(k * EXT + LO - 3 + r, 8, stride=EXT), :] = xr[
                    EAST, f, pl.ds(r * nz + k, 8), :
                ]
                exts[f][pl.ds(k * EXT + LO + bx + r, 8, stride=EXT), :] = xr[
                    WEST, f, pl.ds(r * nz + k, 8), :
                ]

    def advect_x(k, carry):
        acc_p, acc_v = carry
        n = bx + 8
        c = u_ext[ext_at(k, LO, n), :] * scale
        wet = t0 <= k
        res = []
        for f in range(4):
            sh = [exts[f][ext_at(k, LO + o, n), :] for o in (-3, -2, -1, 0, 1, 2)]
            flux = stencil(c, *sh)
            nxt = pltpu.roll(flux, n - 1, 0)[:bx]
            res.append(jnp.where(wet, tend[f, slab(k), :] - (nxt - flux[:bx]), 0.0))
        u_ext[own(k), :] = res[0]
        v_ext[own(k), :] = res[1]
        w_buf[slab(k + 1), :] = res[2]
        p_ext[own(k), :] = res[3]
        pick = (lane >> 1) == k
        acc_p = jnp.where(pick, pltpu.roll(res[3], 2 * k + 1, 1), acc_p)
        acc_v = jnp.where(pick, pltpu.roll(res[1], 2 * k + 1, 1), acc_v)
        return acc_p, acc_v

    acc_p, acc_v = lax.fori_loop(0, nz, advect_x, (zero, zero))

    def send_p(s, acc):
        for n, x in enumerate(edge(p_ext, LO)):
            ps_x[WEST, s, pl.ds(8 * n, 8), :] = x
        start(WEST, *stp(WEST, s))
        for n, x in enumerate(edge(p_ext, LO + bx - 1)):
            ps_x[EAST, s, pl.ds(8 * n, 8), :] = x
        start(EAST, *stp(EAST, s))
        ps_y[s] = acc
        start(SOUTH, *stp(SOUTH, s))
        start(NORTH, *stp(NORTH, s))

    vs_y[...] = acc_v
    start(SOUTH, *uv(SOUTH))
    for n, x in enumerate(edge(u_ext, LO)):
        us_x[pl.ds(8 * n, 8), :] = x
    start(WEST, *uv(WEST))
    send_p(0, acc_p)

    for f in range(4):
        for d in range(4):
            wait_send(d, *ini(d, f))
    for d in (WEST, SOUTH):
        wait_send(d, *ter(d))
        wait_send(d, *uv(d))
        wait_recv(d, *uv(d))
    uh_x[...] = ur_x[...]
    vh0 = pltpu.roll(vr_y[...], by - 1, 1)
    even = (lane & 1) == 0

    def substep(s, vh):
        for d in range(4):
            wait_recv(d, *stp(d, s))
        for k in range(0, nz, 8):
            at = pl.ds(k, 8)
            p_east = pr_x[WEST, s, at, :]
            p_ext[pl.ds(k * EXT + LO + bx, 8, stride=EXT), :] = p_east
            p_ext[pl.ds(k * EXT + LO - 1, 8, stride=EXT), :] = pr_x[EAST, s, at, :]
            uh = uh_x[at, :]
            u_ext[pl.ds(k * EXT + LO + bx, 8, stride=EXT), :] = uh
            wet = wet_x[at, :]
            un = wet * (uh - HC * (p_east - ps_x[EAST, s, at, :]))
            uh_x[at, :] = un - relax_hx * (un - wet * ub_x[at, :])
        vn_h = wet_y * (vh - HC * (pltpu.roll(pr_y[SOUTH - 2, s], by - 1, 1) - ps_y[s]))
        vh_next = vn_h - relax_hy * (vn_h - wet_y * vb_y)
        halo = jnp.where(even, vn_h, pltpu.roll(pr_y[NORTH - 2, s], 1, 1))

        def down(kc, carry):
            q_prev, d_prev = carry
            k0 = kc * CHUNK
            stores = []
            for i in range(CHUNK):
                k = k0 + i
                wet = t0 <= k
                p0 = p_ext[own(k), :]
                pm = p_ext[ext_at(k, LO - 1, bx), :]
                p1 = p_ext[ext_at(k, LO + 1, bx), :]
                un = jnp.where(wet, u_ext[own(k), :] - HC * (p0 - pm), 0.0)
                un1 = jnp.where(t1 <= k, u_ext[ext_at(k, LO + 1, bx), :] - HC * (p1 - p0), 0.0)
                hv = pltpu.roll(halo, by - 1 - 2 * k, 1)
                south = jnp.where(lane == 0, hv, pltpu.roll(p0, 1, 1))
                vn = jnp.where(wet, v_ext[own(k), :] - HC * (p0 - south), 0.0)
                vn1 = jnp.where(lane == by - 1, hv, pltpu.roll(vn, by - 1, 1))
                q = jnp.where(wet, p0 - (g[k] * HC) * ((un1 - un) + (vn1 - vn)), 0.0)
                d_new = (
                    wi[slab(k), :] * (w_buf[slab(k), :] - ZC * (q - q_prev)) - li[slab(k), :] * d_prev
                )
                u_rel = un - relax * (un - jnp.where(wet, prof[0, k], 0.0))
                v_rel = vn - relax * (vn - jnp.where(wet, prof[1, k], 0.0))
                stores.append((k, q, d_new, u_rel, v_rel))
                q_prev, d_prev = q, d_new
            for k, q, d_new, u_rel, v_rel in stores:
                q_buf[slab(k), :] = q
                d_buf[slab(k), :] = d_new
                u_ext[own(k), :] = u_rel
                v_ext[own(k), :] = v_rel
            return q_prev, d_prev

        q_last, d_last = lax.fori_loop(0, nz // CHUNK, down, (zero, zero))
        top = (
            wi[pl.ds(nz * bx, bx), :] * (w_buf[pl.ds(nz * bx, bx), :] + ZC * q_last)
            - li[pl.ds(nz * bx, bx), :] * d_last
        )

        def up(kc, carry):
            x, acc = carry
            k0 = nz - CHUNK - kc * CHUNK
            stores = []
            for i in range(CHUNK - 1, -1, -1):
                k = k0 + i
                below = d_buf[slab(k), :] - cc[slab(k), :] * x
                p = (q_buf[slab(k), :] - (g[k] * ZC) * (x - below)) * keep
                acc = jnp.where((lane >> 1) == k, pltpu.roll(p, (2 * k + 1), 1), acc)
                stores.append((k, p, x * keep))
                x = below
            for k, p, w in stores:
                p_ext[own(k), :] = p
                w_buf[slab(k + 1), :] = w
            return x, acc

        _, acc = lax.fori_loop(0, nz // CHUNK, up, (top, zero))

        for d in range(4):
            wait_send(d, *stp(d, s))

        @pl.when(s < SUB - 1)
        def _():
            send_p(s + 1, acc)

        return vh_next

    lax.fori_loop(0, SUB, substep, vh0)

    def finish(k, carry):
        u_out[slab(k), :] = u_ext[own(k), :]
        v_out[slab(k), :] = v_ext[own(k), :]
        w_out[slab(k), :] = w_buf[slab(k + 1), :]
        p_out[slab(k), :] = p_ext[own(k), :]
        return carry

    lax.fori_loop(0, nz, finish, 0, unroll=4)


def solution(mesh):
    cnt = (mesh.shape["gx"], mesh.shape["gy"])

    def on_device(u, v, w, p, terr, zone, g, prof):
        nz, bx, by = u.shape
        assert by == 128 and bx % 8 == 0 and 2 * nz == by
        flat = [a.reshape(nz * bx, by) for a in (u, v, w, p)]
        f32 = jnp.float32
        vm = pltpu.VMEM
        ext = vm((nz * EXT + 8, by), f32)
        lev = vm((nz * bx, by), f32)
        lev1 = vm(((nz + 1) * bx, by), f32)
        strip = nz * 8 * bx // by
        dma = pltpu.SemaphoreType.DMA
        scratch = [
            ext, ext, ext, ext,
            vm((4, nz * bx, by), f32),
            lev, lev1, lev1, lev1, lev1, lev1,
            vm((2, 4, 3 * nz, by), f32),
            vm((2, 4, 3 * nz, by), f32),
            vm((2, 4, strip, by), f32),
            vm((2, 4, strip, by), f32),
            vm((4, strip, by), f32),
            vm((4, strip, by), f32),
            vm((8, by), jnp.int32),
            vm((bx, by), jnp.int32),
            vm((bx + 8, by), jnp.int32),
            vm((2, SUB, nz, by), f32),
            vm((2, SUB, nz, by), f32),
            vm((SUB, bx, by), f32),
            vm((2, SUB, bx, by), f32),
            vm((nz, by), f32),
            vm((nz, by), f32),
            vm((bx, by), f32),
            vm((bx, by), f32),
            vm((nz, by), f32),
            vm((nz, by), f32),
            vm((nz, by), f32),
            dma((4, 4)), dma((4, 4)),
            dma((2,)), dma((2,)),
            dma((2,)), dma((2,)),
            dma((4, SUB)), dma((4, SUB)),
        ]
        vspec = pl.BlockSpec(memory_space=pltpu.VMEM)
        sspec = pl.BlockSpec(memory_space=pltpu.SMEM)
        outs = pl.pallas_call(
            functools.partial(kernel, nz, bx, cnt),
            out_shape=[jax.ShapeDtypeStruct((nz * bx, by), f32)] * 4,
            in_specs=[vspec] * 5 + [sspec] * 3,
            out_specs=[vspec] * 4,
            scratch_shapes=scratch,
            compiler_params=pltpu.CompilerParams(collective_id=0, has_side_effects=True),
        )(*flat, terr, zone, g, prof)
        return tuple(a.reshape(nz, bx, by) for a in outs)

    field = P(None, "gx", "gy")
    return jax.shard_map(
        on_device,
        mesh=mesh,
        in_specs=(field, field, field, field, P("gx", "gy"), P(), P(), P()),
        out_specs=(field,) * 4,
        check_vma=False,
    )
```

```python
import functools

import jax
import jax.numpy as jnp
from jax import lax
from jax.experimental import pallas as pl
from jax.experimental.pallas import tpu as pltpu
from jax.sharding import PartitionSpec as P

SUB = 6
ADV = 0.3
HC = 0.4
ZC = 1.0
RELAX = 0.5
EXT = 32
LO = 8
DRY = 1 << 20
WEST, EAST, SOUTH, NORTH = 0, 1, 2, 3
CHUNK = 32


def stencil(c, m3, m2, m1, f0, e1, e2):
    centered = 37.0 * (f0 + m1) - 8.0 * (e1 + m2) + (e2 + m3)
    upwind = 10.0 * (f0 - m1) - 5.0 * (e1 - m2) + (e2 - m3)
    return c * centered - jnp.abs(c) * upwind


def kernel(
    nz,
    bx,
    cnt,
    u_in,
    v_in,
    w_in,
    p_in,
    terr,
    zone,
    g,
    prof,
    u_out,
    v_out,
    w_out,
    p_out,
    u_ext,
    v_ext,
    w_ext,
    p_ext,
    tend,
    q_buf,
    d_buf,
    w_buf,
    cc,
    li,
    wi,
    xs,
    xr,
    ys,
    yr,
    g_lo,
    g_hi,
    trx,
    tr_y,
    terr_ext,
    ps_x,
    pr_x,
    ps_y,
    pr_y,
    us_x,
    ur_x,
    vs_y,
    vr_y,
    ub_x,
    wet_x,
    uh_x,
    ini_s,
    ini_r,
    ter_s,
    ter_r,
    uv_s,
    uv_r,
    stp_s,
    stp_r,
):
    by = 128
    gx = lax.axis_index("gx")
    gy = lax.axis_index("gy")
    nx_dev, ny_dev = cnt
    has = (gx > 0, gx < nx_dev - 1, gy > 0, gy < ny_dev - 1)
    peer = ({"gx": gx - 1}, {"gx": gx + 1}, {"gy": gy - 1}, {"gy": gy + 1})
    opp = (EAST, WEST, NORTH, SOUTH)
    exts = (u_ext, v_ext, w_ext, p_ext)
    ins = (u_in, v_in, w_in, p_in)

    barrier = pltpu.get_barrier_semaphore()
    for d in range(4):

        @pl.when(has[d])
        def _(d=d):
            pl.semaphore_signal(
                barrier, inc=1, device_id=peer[d], device_id_type=pl.DeviceIdType.MESH
            )

    def rcopy(d, src, dst, ss, rs):
        return pltpu.make_async_remote_copy(
            src_ref=src,
            dst_ref=dst,
            send_sem=ss,
            recv_sem=rs,
            device_id=peer[d],
            device_id_type=pl.DeviceIdType.MESH,
        )

    def start(d, *args):
        @pl.when(has[d])
        def _():
            rcopy(d, *args).start()

    def wait_send(d, *args):
        @pl.when(has[d])
        def _():
            rcopy(d, *args).wait_send()

    def wait_recv(d, *args):
        @pl.when(has[opp[d]])
        def _():
            rcopy(d, *args).wait_recv()

    def ini(d, f):
        if d < 2:
            return xs.at[d, f], xr.at[d, f], ini_s.at[d, f], ini_r.at[d, f]
        return ys.at[d - 2, f], yr.at[d - 2, f], ini_s.at[d, f], ini_r.at[d, f]

    def ter(d):
        if d == WEST:
            return terr.at[pl.ds(0, 8)], trx, ter_s.at[0], ter_r.at[0]
        return terr, tr_y, ter_s.at[1], ter_r.at[1]

    def uv(d):
        if d == WEST:
            return us_x, ur_x, uv_s.at[0], uv_r.at[0]
        return vs_y, vr_y, uv_s.at[1], uv_r.at[1]

    def stp(d, s):
        if d < 2:
            return ps_x.at[d, s], pr_x.at[d, s], stp_s.at[d, s], stp_r.at[d, s]
        return ps_y.at[s], pr_y.at[d - 2, s], stp_s.at[d, s], stp_r.at[d, s]

    rows = lax.broadcasted_iota(jnp.int32, (bx, by), 0)
    lane = lax.broadcasted_iota(jnp.int32, (bx, by), 1)

    def slab(k):
        return pl.ds(pl.multiple_of(k * bx, bx), bx)

    def ext_at(k, off, n):
        return pl.ds(k * EXT + off, n)

    def own(k):
        return pl.ds(pl.multiple_of(k * EXT + LO, 8), bx)

    def edge(ref, off):
        return [ref[pl.ds(k * EXT + off, 8, stride=EXT), :] for k in range(0, nz, 8)]

    for d in range(4):

        @pl.when(jnp.logical_not(has[opp[d]]))
        def _(d=d):
            if d < 2:
                xr[d] = jnp.zeros(xr.shape[1:], jnp.float32)
                pr_x[d] = jnp.zeros(pr_x.shape[1:], jnp.float32)
            else:
                yr[d - 2] = jnp.zeros(yr.shape[1:], jnp.float32)
                pr_y[d - 2] = jnp.zeros(pr_y.shape[1:], jnp.float32)
            if d == WEST:
                trx[...] = jnp.full(trx.shape, DRY, jnp.int32)
                ur_x[...] = jnp.zeros(ur_x.shape, jnp.float32)
            if d == SOUTH:
                tr_y[...] = jnp.full(tr_y.shape, DRY, jnp.int32)
                vr_y[...] = jnp.zeros(vr_y.shape, jnp.float32)

    neighbours = sum(h.astype(jnp.int32) for h in has)
    pl.semaphore_wait(barrier, neighbours)
    start(WEST, *ter(WEST))
    start(SOUTH, *ter(SOUTH))

    for f in range(4):
        for r in range(3):
            for k in range(0, nz, 8):
                xs[WEST, f, pl.ds(r * nz + k, 8), :] = ins[f][pl.ds(k * bx + r, 8, stride=bx), :]
                xs[EAST, f, pl.ds(r * nz + k, 8), :] = ins[f][
                    pl.ds(k * bx + bx - 3 + r, 8, stride=bx), :
                ]
        start(WEST, *ini(WEST, f))
        start(EAST, *ini(EAST, f))

    group = by // 8
    for f in range(4):

        def pack(kg, carry, f=f):
            lo = hi = jnp.zeros((bx, by), jnp.float32)
            for kk in range(group):
                k = kg * group + kk
                x = ins[f][slab(k), :]
                exts[f][own(k), :] = x
                pick = (lane >> 3) == kk
                lo = jnp.where(pick, pltpu.roll(x, 8 * kk + 3, 1), lo)
                hi = jnp.where(pick, pltpu.roll(x, 8 * kk + 5, 1), hi)
            ys[SOUTH - 2, f, slab(kg), :] = lo
            ys[NORTH - 2, f, slab(kg), :] = hi
            return carry

        lax.fori_loop(0, nz // group, pack, 0)
        start(SOUTH, *ini(SOUTH, f))
        start(NORTH, *ini(NORTH, f))

    def relax_of(ci, rj):
        best = None
        for n, dist in enumerate(
            (
                ci,
                (nx_dev * bx - 1.0) - ci,
                rj,
                (ny_dev * by - 1.0) - rj,
            )
        ):
            width = jnp.full(ci.shape, zone[n], jnp.int32).astype(jnp.float32)
            ramp = jnp.maximum(width - dist, 0.0) / width
            best = ramp if best is None else jnp.maximum(best, ramp)
        return RELAX * best

    start_x = gx * bx
    start_y = gy * by
    ci = (rows + start_x).astype(jnp.float32)
    rj = (lane + start_y).astype(jnp.float32)
    relax = relax_of(ci, rj)
    keep = 1.0 - relax
    relax_hx = relax_of(
        (jnp.zeros((8, by), jnp.int32) + (start_x + bx)).astype(jnp.float32), rj[:8]
    )
    relax_hy = relax_of(ci, (jnp.zeros((bx, by), jnp.int32) + (start_y + by)).astype(jnp.float32))

    zero = jnp.zeros((bx, by), jnp.float32)
    for ref in (cc, li, wi, d_buf, w_buf):
        ref[pl.ds(0, bx), :] = zero
    t0 = terr[...]

    def coeff(k, carry):
        c_prev, vrow = carry
        above = jnp.minimum(k + 1, nz - 1)
        wet = jnp.where(t0 <= k, 1.0, 0.0)
        wet_b = jnp.where(jnp.logical_and(t0 <= k - 1, rows + k > rows), 1.0, 0.0)
        wet_a = jnp.where(jnp.logical_and(t0 <= k + 1, rows + (k + 1) < rows + nz), 1.0, 0.0)
        gk = (ZC * ZC) * g[k] * wet
        ga = (ZC * ZC) * g[above] * wet_a
        low = -gk * wet_b
        up = -ga * wet
        inv = 1.0 / (1.0 + wet * (ga + gk) - low * c_prev)
        c_new = up * inv
        cc[slab(k + 1), :] = c_new
        li[slab(k + 1), :] = low * inv
        wi[slab(k + 1), :] = wet * inv
        ub_x[pl.ds(k, 1), :] = jnp.full((1, by), prof[0, k], jnp.float32)
        vrow = jnp.where((lane >> 1) == k, prof[1, k], vrow)
        return c_new, vrow

    _, vb_y = lax.fori_loop(0, nz, coeff, (zero, zero))

    wait_recv(WEST, *ter(WEST))
    wait_recv(SOUTH, *ter(SOUTH))
    terr_ext[pl.ds(0, bx), :] = t0
    terr_ext[pl.ds(bx, 8), :] = trx[...]
    t1 = terr_ext[pl.ds(1, bx), :]
    t_east = jnp.broadcast_to(trx[0:1, :], (8, by))
    sub8 = lax.broadcasted_iota(jnp.int32, (8, by), 0)
    for k in range(0, nz, 8):
        wet_x[pl.ds(k, 8), :] = jnp.where(t_east <= sub8 + k, 1.0, 0.0)
    t_north = jnp.broadcast_to(tr_y[:, 0:1], (bx, by))
    wet_y = jnp.where(t_north <= (lane >> 1), 1.0, 0.0)

    scale = ADV / 60.0
    for f in range(4):
        wait_recv(SOUTH, *ini(SOUTH, f))
        wait_recv(NORTH, *ini(NORTH, f))

    def shifts(xw, xe):
        return (
            pltpu.roll(xw, 3, 1),
            pltpu.roll(xw, 2, 1),
            pltpu.roll(xw, 1, 1),
            xw,
            pltpu.roll(xe, by - 1, 1),
            pltpu.roll(xe, by - 2, 1),
        )

    def merge(kg, carry):
        at = slab(kg)

        def low(f):
            return jnp.where(
                (lane & 7) < 3,
                pltpu.roll(yr[NORTH - 2, f, at, :], by - 2, 1),
                ys[SOUTH - 2, f, at, :],
            )

        def high(f):
            return jnp.where(
                (lane & 7) < 5, ys[NORTH - 2, f, at, :], pltpu.roll(yr[SOUTH - 2, f, at, :], 2, 1)
            )

        c_lo = low(1) * scale
        c_hi = high(1) * scale
        for f in range(4):
            x = low(f)
            g_lo[f, at, :] = stencil(c_lo, *shifts(x, x))
            x = high(f)
            g_hi[f, at, :] = stencil(c_hi, *shifts(x, x))
        return carry

    lax.fori_loop(0, nz // group, merge, 0)

    def advect_y(k, carry):
        kg = k // group
        kk = k - kg * group
        c = v_ext[own(k), :] * scale
        for f in range(4):
            x = exts[f][own(k), :]
            lo = pltpu.roll(g_lo[f, slab(kg), :], by - 3 - 8 * kk, 1)
            hi = pltpu.roll(g_hi[f, slab(kg), :], by - 5 - 8 * kk, 1)
            flux = stencil(c, *shifts(x, x))
            flux = jnp.where(lane >= by - 2, hi, jnp.where(lane < 3, lo, flux))
            nxt = pltpu.roll(jnp.where(lane == 0, hi, flux), by - 1, 1)
            tend[f, slab(k), :] = x - (nxt - flux)
        return carry

    lax.fori_loop(0, nz, advect_y, 0, unroll=2)

    for f in range(4):
        wait_recv(WEST, *ini(WEST, f))
        wait_recv(EAST, *ini(EAST, f))
        for r in range(3):
            for k in range(0, nz, 8):
                exts[f][pl.ds(k * EXT + LO - 3 + r, 8, stride=EXT), :] = xr[
                    EAST, f, pl.ds(r * nz + k, 8), :
                ]
                exts[f][pl.ds(k * EXT + LO + bx + r, 8, stride=EXT), :] = xr[
                    WEST, f, pl.ds(r * nz + k, 8), :
                ]

    def advect_x(k, carry):
        acc_p, acc_v = carry
        n = bx + 8
        c = u_ext[ext_at(k, LO, n), :] * scale
        wet = t0 <= k
        res = []
        for f in range(4):
            sh = [exts[f][ext_at(k, LO + o, n), :] for o in (-3, -2, -1, 0, 1, 2)]
            flux = stencil(c, *sh)
            nxt = pltpu.roll(flux, n - 1, 0)[:bx]
            res.append(jnp.where(wet, tend[f, slab(k), :] - (nxt - flux[:bx]), 0.0))
        u_ext[own(k), :] = res[0]
        v_ext[own(k), :] = res[1]
        w_buf[slab(k + 1), :] = res[2]
        p_ext[own(k), :] = res[3]
        pick = (lane >> 1) == k
        acc_p = jnp.where(pick, pltpu.roll(res[3], 2 * k + 1, 1), acc_p)
        acc_v = jnp.where(pick, pltpu.roll(res[1], 2 * k + 1, 1), acc_v)
        return acc_p, acc_v

    acc_p, acc_v = lax.fori_loop(0, nz, advect_x, (zero, zero), unroll=4)

    def send_p(s, acc):
        for n, x in enumerate(edge(p_ext, LO)):
            ps_x[WEST, s, pl.ds(8 * n, 8), :] = x
        start(WEST, *stp(WEST, s))
        for n, x in enumerate(edge(p_ext, LO + bx - 1)):
            ps_x[EAST, s, pl.ds(8 * n, 8), :] = x
        start(EAST, *stp(EAST, s))
        ps_y[s] = acc
        start(SOUTH, *stp(SOUTH, s))
        start(NORTH, *stp(NORTH, s))

    vs_y[...] = acc_v
    start(SOUTH, *uv(SOUTH))
    for n, x in enumerate(edge(u_ext, LO)):
        us_x[pl.ds(8 * n, 8), :] = x
    start(WEST, *uv(WEST))
    send_p(0, acc_p)

    for f in range(4):
        for d in range(4):
            wait_send(d, *ini(d, f))
    for d in (WEST, SOUTH):
        wait_send(d, *ter(d))
        wait_send(d, *uv(d))
        wait_recv(d, *uv(d))
    uh_x[...] = ur_x[...]
    vh0 = pltpu.roll(vr_y[...], by - 1, 1)
    even = (lane & 1) == 0

    def substep(s, vh):
        for d in range(4):
            wait_recv(d, *stp(d, s))
        for k in range(0, nz, 8):
            at = pl.ds(k, 8)
            p_east = pr_x[WEST, s, at, :]
            p_ext[pl.ds(k * EXT + LO + bx, 8, stride=EXT), :] = p_east
            p_ext[pl.ds(k * EXT + LO - 1, 8, stride=EXT), :] = pr_x[EAST, s, at, :]
            uh = uh_x[at, :]
            u_ext[pl.ds(k * EXT + LO + bx, 8, stride=EXT), :] = uh
            wet = wet_x[at, :]
            un = wet * (uh - HC * (p_east - ps_x[EAST, s, at, :]))
            uh_x[at, :] = un - relax_hx * (un - wet * ub_x[at, :])
        vn_h = wet_y * (vh - HC * (pltpu.roll(pr_y[SOUTH - 2, s], by - 1, 1) - ps_y[s]))
        vh_next = vn_h - relax_hy * (vn_h - wet_y * vb_y)
        halo = jnp.where(even, vn_h, pltpu.roll(pr_y[NORTH - 2, s], 1, 1))

        def down(kc, carry):
            q_prev, d_prev = carry
            k0 = kc * CHUNK
            stores = []
            for i in range(CHUNK):
                k = k0 + i
                wet = t0 <= k
                p0 = p_ext[own(k), :]
                pm = p_ext[ext_at(k, LO - 1, bx), :]
                p1 = p_ext[ext_at(k, LO + 1, bx), :]
                un = jnp.where(wet, u_ext[own(k), :] - HC * (p0 - pm), 0.0)
                un1 = jnp.where(t1 <= k, u_ext[ext_at(k, LO + 1, bx), :] - HC * (p1 - p0), 0.0)
                hv = pltpu.roll(halo, by - 1 - 2 * k, 1)
                south = jnp.where(lane == 0, hv, pltpu.roll(p0, 1, 1))
                vn = jnp.where(wet, v_ext[own(k), :] - HC * (p0 - south), 0.0)
                vn1 = jnp.where(lane == by - 1, hv, pltpu.roll(vn, by - 1, 1))
                q = jnp.where(wet, p0 - (g[k] * HC) * ((un1 - un) + (vn1 - vn)), 0.0)
                d_new = (
                    wi[slab(k), :] * (w_buf[slab(k), :] - ZC * (q - q_prev)) - li[slab(k), :] * d_prev
                )
                u_rel = un - relax * (un - jnp.where(wet, prof[0, k], 0.0))
                v_rel = vn - relax * (vn - jnp.where(wet, prof[1, k], 0.0))
                stores.append((k, q, d_new, u_rel, v_rel))
                q_prev, d_prev = q, d_new
            for k, q, d_new, u_rel, v_rel in stores:
                q_buf[slab(k), :] = q
                d_buf[slab(k), :] = d_new
                u_ext[own(k), :] = u_rel
                v_ext[own(k), :] = v_rel
            return q_prev, d_prev

        q_last, d_last = lax.fori_loop(0, nz // CHUNK, down, (zero, zero))
        top = (
            wi[pl.ds(nz * bx, bx), :] * (w_buf[pl.ds(nz * bx, bx), :] + ZC * q_last)
            - li[pl.ds(nz * bx, bx), :] * d_last
        )

        def up(kc, carry):
            x, acc = carry
            k0 = nz - CHUNK - kc * CHUNK
            stores = []
            for i in range(CHUNK - 1, -1, -1):
                k = k0 + i
                below = d_buf[slab(k), :] - cc[slab(k), :] * x
                p = (q_buf[slab(k), :] - (g[k] * ZC) * (x - below)) * keep
                acc = jnp.where((lane >> 1) == k, pltpu.roll(p, (2 * k + 1), 1), acc)
                stores.append((k, p, x * keep))
                x = below
            for k, p, w in stores:
                p_ext[own(k), :] = p
                w_buf[slab(k + 1), :] = w
            return x, acc

        _, acc = lax.fori_loop(0, nz // CHUNK, up, (top, zero))

        for d in range(4):
            wait_send(d, *stp(d, s))

        @pl.when(s < SUB - 1)
        def _():
            send_p(s + 1, acc)

        return vh_next

    lax.fori_loop(0, SUB, substep, vh0)

    def finish(k, carry):
        u_out[slab(k), :] = u_ext[own(k), :]
        v_out[slab(k), :] = v_ext[own(k), :]
        w_out[slab(k), :] = w_buf[slab(k + 1), :]
        p_out[slab(k), :] = p_ext[own(k), :]
        return carry

    lax.fori_loop(0, nz, finish, 0, unroll=4)


def solution(mesh):
    cnt = (mesh.shape["gx"], mesh.shape["gy"])

    def on_device(u, v, w, p, terr, zone, g, prof):
        nz, bx, by = u.shape
        assert by == 128 and bx % 8 == 0 and 2 * nz == by
        flat = [a.reshape(nz * bx, by) for a in (u, v, w, p)]
        f32 = jnp.float32
        vm = pltpu.VMEM
        ext = vm((nz * EXT + 8, by), f32)
        lev = vm((nz * bx, by), f32)
        lev1 = vm(((nz + 1) * bx, by), f32)
        strip = nz * 8 * bx // by
        dma = pltpu.SemaphoreType.DMA
        scratch = [
            ext, ext, ext, ext,
            vm((4, nz * bx, by), f32),
            lev, lev1, lev1, lev1, lev1, lev1,
            vm((2, 4, 3 * nz, by), f32),
            vm((2, 4, 3 * nz, by), f32),
            vm((2, 4, strip, by), f32),
            vm((2, 4, strip, by), f32),
            vm((4, strip, by), f32),
            vm((4, strip, by), f32),
            vm((8, by), jnp.int32),
            vm((bx, by), jnp.int32),
            vm((bx + 8, by), jnp.int32),
            vm((2, SUB, nz, by), f32),
            vm((2, SUB, nz, by), f32),
            vm((SUB, bx, by), f32),
            vm((2, SUB, bx, by), f32),
            vm((nz, by), f32),
            vm((nz, by), f32),
            vm((bx, by), f32),
            vm((bx, by), f32),
            vm((nz, by), f32),
            vm((nz, by), f32),
            vm((nz, by), f32),
            dma((4, 4)), dma((4, 4)),
            dma((2,)), dma((2,)),
            dma((2,)), dma((2,)),
            dma((4, SUB)), dma((4, SUB)),
        ]
        vspec = pl.BlockSpec(memory_space=pltpu.VMEM)
        sspec = pl.BlockSpec(memory_space=pltpu.SMEM)
        outs = pl.pallas_call(
            functools.partial(kernel, nz, bx, cnt),
            out_shape=[jax.ShapeDtypeStruct((nz * bx, by), f32)] * 4,
            in_specs=[vspec] * 5 + [sspec] * 3,
            out_specs=[vspec] * 4,
            scratch_shapes=scratch,
            compiler_params=pltpu.CompilerParams(collective_id=0, has_side_effects=True),
        )(*flat, terr, zone, g, prof)
        return tuple(a.reshape(nz, bx, by) for a in outs)

    field = P(None, "gx", "gy")
    return jax.shard_map(
        on_device,
        mesh=mesh,
        in_specs=(field, field, field, field, P("gx", "gy"), P(), P(), P()),
        out_specs=(field,) * 4,
        check_vma=False,
    )
```

```python
import functools

import jax
import jax.numpy as jnp
from jax import lax
from jax.experimental import pallas as pl
from jax.experimental.pallas import tpu as pltpu
from jax.sharding import PartitionSpec as P

SUB = 6
ADV = 0.3
HC = 0.4
ZC = 1.0
RELAX = 0.5
EXT = 32
LO = 8
DRY = 1 << 20
WEST, EAST, SOUTH, NORTH = 0, 1, 2, 3
CHUNK = 32


def stencil(c, m3, m2, m1, f0, e1, e2):
    centered = 37.0 * (f0 + m1) - 8.0 * (e1 + m2) + (e2 + m3)
    upwind = 10.0 * (f0 - m1) - 5.0 * (e1 - m2) + (e2 - m3)
    return c * centered - jnp.abs(c) * upwind


def kernel(
    nz,
    bx,
    cnt,
    u_in,
    v_in,
    w_in,
    p_in,
    terr,
    zone,
    g,
    prof,
    u_out,
    v_out,
    w_out,
    p_out,
    u_ext,
    v_ext,
    w_ext,
    p_ext,
    tend,
    q_buf,
    d_buf,
    w_buf,
    cc,
    li,
    wi,
    xs,
    xr,
    ys,
    yr,
    g_lo,
    g_hi,
    trx,
    tr_y,
    terr_ext,
    ps_x,
    pr_x,
    ps_y,
    pr_y,
    us_x,
    ur_x,
    vs_y,
    vr_y,
    ub_x,
    wet_x,
    uh_x,
    ini_s,
    ini_r,
    ter_s,
    ter_r,
    uv_s,
    uv_r,
    stp_s,
    stp_r,
):
    by = 128
    gx = lax.axis_index("gx")
    gy = lax.axis_index("gy")
    nx_dev, ny_dev = cnt
    has = (gx > 0, gx < nx_dev - 1, gy > 0, gy < ny_dev - 1)
    peer = ({"gx": gx - 1}, {"gx": gx + 1}, {"gy": gy - 1}, {"gy": gy + 1})
    opp = (EAST, WEST, NORTH, SOUTH)
    exts = (u_ext, v_ext, w_ext, p_ext)
    ins = (u_in, v_in, w_in, p_in)

    barrier = pltpu.get_barrier_semaphore()
    for d in range(4):

        @pl.when(has[d])
        def _(d=d):
            pl.semaphore_signal(
                barrier, inc=1, device_id=peer[d], device_id_type=pl.DeviceIdType.MESH
            )

    def rcopy(d, src, dst, ss, rs):
        return pltpu.make_async_remote_copy(
            src_ref=src,
            dst_ref=dst,
            send_sem=ss,
            recv_sem=rs,
            device_id=peer[d],
            device_id_type=pl.DeviceIdType.MESH,
        )

    def start(d, *args):
        @pl.when(has[d])
        def _():
            rcopy(d, *args).start()

    def wait_send(d, *args):
        @pl.when(has[d])
        def _():
            rcopy(d, *args).wait_send()

    def wait_recv(d, *args):
        @pl.when(has[opp[d]])
        def _():
            rcopy(d, *args).wait_recv()

    def ini(d, f):
        if d < 2:
            return xs.at[d, f], xr.at[d, f], ini_s.at[d, f], ini_r.at[d, f]
        return ys.at[d - 2, f], yr.at[d - 2, f], ini_s.at[d, f], ini_r.at[d, f]

    def ter(d):
        if d == WEST:
            return terr.at[pl.ds(0, 8)], trx, ter_s.at[0], ter_r.at[0]
        return terr, tr_y, ter_s.at[1], ter_r.at[1]

    def uv(d):
        if d == WEST:
            return us_x, ur_x, uv_s.at[0], uv_r.at[0]
        return vs_y, vr_y, uv_s.at[1], uv_r.at[1]

    def stp(d, s, h=0):
        sems = stp_s.at[d, s, h], stp_r.at[d, s, h]
        if d < 2:
            part = pl.ds(h * CHUNK, CHUNK)
            return ps_x.at[d, s, part], pr_x.at[d, s, part], *sems
        return ps_y.at[s], pr_y.at[d - 2, s], *sems

    def parts(d):
        return range(nz // CHUNK if d < 2 else 1)

    rows = lax.broadcasted_iota(jnp.int32, (bx, by), 0)
    lane = lax.broadcasted_iota(jnp.int32, (bx, by), 1)

    def slab(k):
        return pl.ds(pl.multiple_of(k * bx, bx), bx)

    def ext_at(k, off, n):
        return pl.ds(k * EXT + off, n)

    def own(k):
        return pl.ds(pl.multiple_of(k * EXT + LO, 8), bx)

    def edge(ref, off):
        return [ref[pl.ds(k * EXT + off, 8, stride=EXT), :] for k in range(0, nz, 8)]

    for d in range(4):

        @pl.when(jnp.logical_not(has[opp[d]]))
        def _(d=d):
            if d < 2:
                xr[d] = jnp.zeros(xr.shape[1:], jnp.float32)
                pr_x[d] = jnp.zeros(pr_x.shape[1:], jnp.float32)
            else:
                yr[d - 2] = jnp.zeros(yr.shape[1:], jnp.float32)
                pr_y[d - 2] = jnp.zeros(pr_y.shape[1:], jnp.float32)
            if d == WEST:
                trx[...] = jnp.full(trx.shape, DRY, jnp.int32)
                ur_x[...] = jnp.zeros(ur_x.shape, jnp.float32)
            if d == SOUTH:
                tr_y[...] = jnp.full(tr_y.shape, DRY, jnp.int32)
                vr_y[...] = jnp.zeros(vr_y.shape, jnp.float32)

    neighbours = sum(h.astype(jnp.int32) for h in has)
    pl.semaphore_wait(barrier, neighbours)
    start(WEST, *ter(WEST))
    start(SOUTH, *ter(SOUTH))

    for f in range(4):
        for r in range(3):
            for k in range(0, nz, 8):
                xs[WEST, f, pl.ds(r * nz + k, 8), :] = ins[f][pl.ds(k * bx + r, 8, stride=bx), :]
                xs[EAST, f, pl.ds(r * nz + k, 8), :] = ins[f][
                    pl.ds(k * bx + bx - 3 + r, 8, stride=bx), :
                ]
        start(WEST, *ini(WEST, f))
        start(EAST, *ini(EAST, f))

    group = by // 8
    for f in range(4):

        def pack(kg, carry, f=f):
            lo = hi = jnp.zeros((bx, by), jnp.float32)
            for kk in range(group):
                k = kg * group + kk
                x = ins[f][slab(k), :]
                exts[f][own(k), :] = x
                pick = (lane >> 3) == kk
                lo = jnp.where(pick, pltpu.roll(x, 8 * kk + 3, 1), lo)
                hi = jnp.where(pick, pltpu.roll(x, 8 * kk + 5, 1), hi)
            ys[SOUTH - 2, f, slab(kg), :] = lo
            ys[NORTH - 2, f, slab(kg), :] = hi
            return carry

        lax.fori_loop(0, nz // group, pack, 0)
        start(SOUTH, *ini(SOUTH, f))
        start(NORTH, *ini(NORTH, f))

    def relax_of(ci, rj):
        best = None
        for n, dist in enumerate(
            (
                ci,
                (nx_dev * bx - 1.0) - ci,
                rj,
                (ny_dev * by - 1.0) - rj,
            )
        ):
            width = jnp.full(ci.shape, zone[n], jnp.int32).astype(jnp.float32)
            ramp = jnp.maximum(width - dist, 0.0) / width
            best = ramp if best is None else jnp.maximum(best, ramp)
        return RELAX * best

    start_x = gx * bx
    start_y = gy * by
    ci = (rows + start_x).astype(jnp.float32)
    rj = (lane + start_y).astype(jnp.float32)
    relax = relax_of(ci, rj)
    keep = 1.0 - relax
    relax_hx = relax_of(
        (jnp.zeros((8, by), jnp.int32) + (start_x + bx)).astype(jnp.float32), rj[:8]
    )
    relax_hy = relax_of(ci, (jnp.zeros((bx, by), jnp.int32) + (start_y + by)).astype(jnp.float32))

    zero = jnp.zeros((bx, by), jnp.float32)
    for ref in (cc, li, wi, d_buf, w_buf):
        ref[pl.ds(0, bx), :] = zero
    t0 = terr[...]

    def coeff(k, carry):
        c_prev, vrow = carry
        above = jnp.minimum(k + 1, nz - 1)
        wet = jnp.where(t0 <= k, 1.0, 0.0)
        wet_b = jnp.where(jnp.logical_and(t0 <= k - 1, rows + k > rows), 1.0, 0.0)
        wet_a = jnp.where(jnp.logical_and(t0 <= k + 1, rows + (k + 1) < rows + nz), 1.0, 0.0)
        gk = (ZC * ZC) * g[k] * wet
        ga = (ZC * ZC) * g[above] * wet_a
        low = -gk * wet_b
        up = -ga * wet
        inv = 1.0 / (1.0 + wet * (ga + gk) - low * c_prev)
        c_new = up * inv
        cc[slab(k + 1), :] = c_new
        li[slab(k + 1), :] = low * inv
        wi[slab(k + 1), :] = wet * inv
        ub_x[pl.ds(k, 1), :] = jnp.full((1, by), prof[0, k], jnp.float32)
        vrow = jnp.where((lane >> 1) == k, prof[1, k], vrow)
        return c_new, vrow

    _, vb_y = lax.fori_loop(0, nz, coeff, (zero, zero))

    wait_recv(WEST, *ter(WEST))
    wait_recv(SOUTH, *ter(SOUTH))
    terr_ext[pl.ds(0, bx), :] = t0
    terr_ext[pl.ds(bx, 8), :] = trx[...]
    t1 = terr_ext[pl.ds(1, bx), :]
    t_east = jnp.broadcast_to(trx[0:1, :], (8, by))
    sub8 = lax.broadcasted_iota(jnp.int32, (8, by), 0)
    for k in range(0, nz, 8):
        wet_x[pl.ds(k, 8), :] = jnp.where(t_east <= sub8 + k, 1.0, 0.0)
    t_north = jnp.broadcast_to(tr_y[:, 0:1], (bx, by))
    wet_y = jnp.where(t_north <= (lane >> 1), 1.0, 0.0)

    scale = ADV / 60.0
    for f in range(4):
        wait_recv(SOUTH, *ini(SOUTH, f))
        wait_recv(NORTH, *ini(NORTH, f))

    def shifts(xw, xe):
        return (
            pltpu.roll(xw, 3, 1),
            pltpu.roll(xw, 2, 1),
            pltpu.roll(xw, 1, 1),
            xw,
            pltpu.roll(xe, by - 1, 1),
            pltpu.roll(xe, by - 2, 1),
        )

    def merge(kg, carry):
        at = slab(kg)

        def low(f):
            return jnp.where(
                (lane & 7) < 3,
                pltpu.roll(yr[NORTH - 2, f, at, :], by - 2, 1),
                ys[SOUTH - 2, f, at, :],
            )

        def high(f):
            return jnp.where(
                (lane & 7) < 5, ys[NORTH - 2, f, at, :], pltpu.roll(yr[SOUTH - 2, f, at, :], 2, 1)
            )

        c_lo = low(1) * scale
        c_hi = high(1) * scale
        for f in range(4):
            x = low(f)
            g_lo[f, at, :] = stencil(c_lo, *shifts(x, x))
            x = high(f)
            g_hi[f, at, :] = stencil(c_hi, *shifts(x, x))
        return carry

    lax.fori_loop(0, nz // group, merge, 0)

    def advect_y(k, carry):
        kg = k // group
        kk = k - kg * group
        c = v_ext[own(k), :] * scale
        for f in range(4):
            x = exts[f][own(k), :]
            lo = pltpu.roll(g_lo[f, slab(kg), :], by - 3 - 8 * kk, 1)
            hi = pltpu.roll(g_hi[f, slab(kg), :], by - 5 - 8 * kk, 1)
            flux = stencil(c, *shifts(x, x))
            flux = jnp.where(lane >= by - 2, hi, jnp.where(lane < 3, lo, flux))
            nxt = pltpu.roll(jnp.where(lane == 0, hi, flux), by - 1, 1)
            tend[f, slab(k), :] = x - (nxt - flux)
        return carry

    lax.fori_loop(0, nz, advect_y, 0, unroll=2)

    for f in range(4):
        wait_recv(WEST, *ini(WEST, f))
        wait_recv(EAST, *ini(EAST, f))
        for r in range(3):
            for k in range(0, nz, 8):
                exts[f][pl.ds(k * EXT + LO - 3 + r, 8, stride=EXT), :] = xr[
                    EAST, f, pl.ds(r * nz + k, 8), :
                ]
                exts[f][pl.ds(k * EXT + LO + bx + r, 8, stride=EXT), :] = xr[
                    WEST, f, pl.ds(r * nz + k, 8), :
                ]

    def advect_x(k, carry):
        acc_p, acc_v = carry
        n = bx + 8
        c = u_ext[ext_at(k, LO, n), :] * scale
        wet = t0 <= k
        res = []
        for f in range(4):
            sh = [exts[f][ext_at(k, LO + o, n), :] for o in (-3, -2, -1, 0, 1, 2)]
            flux = stencil(c, *sh)
            nxt = pltpu.roll(flux, n - 1, 0)[:bx]
            res.append(jnp.where(wet, tend[f, slab(k), :] - (nxt - flux[:bx]), 0.0))
        u_ext[own(k), :] = res[0]
        v_ext[own(k), :] = res[1]
        w_buf[slab(k + 1), :] = res[2]
        p_ext[own(k), :] = res[3]
        pick = (lane >> 1) == k
        acc_p = jnp.where(pick, pltpu.roll(res[3], 2 * k + 1, 1), acc_p)
        acc_v = jnp.where(pick, pltpu.roll(res[1], 2 * k + 1, 1), acc_v)
        return acc_p, acc_v

    acc_p, acc_v = lax.fori_loop(0, nz, advect_x, (zero, zero), unroll=4)

    def send_x(s, h):
        for d, off in ((WEST, LO), (EAST, LO + bx - 1)):
            for k in range(h * CHUNK, (h + 1) * CHUNK, 8):
                ps_x[d, s, pl.ds(k, 8), :] = p_ext[pl.ds(k * EXT + off, 8, stride=EXT), :]
            start(d, *stp(d, s, h))

    def send_y(s, acc):
        ps_y[s] = acc
        start(SOUTH, *stp(SOUTH, s))
        start(NORTH, *stp(NORTH, s))

    vs_y[...] = acc_v
    start(SOUTH, *uv(SOUTH))
    for n, x in enumerate(edge(u_ext, LO)):
        us_x[pl.ds(8 * n, 8), :] = x
    start(WEST, *uv(WEST))
    for h in range(nz // CHUNK):
        send_x(0, h)
    send_y(0, acc_p)

    for f in range(4):
        for d in range(4):
            wait_send(d, *ini(d, f))
    for d in (WEST, SOUTH):
        wait_send(d, *ter(d))
        wait_send(d, *uv(d))
        wait_recv(d, *uv(d))
    uh_x[...] = ur_x[...]
    vh0 = pltpu.roll(vr_y[...], by - 1, 1)
    even = (lane & 1) == 0

    def substep(s, vh):
        for d in range(4):
            for h in parts(d):
                wait_recv(d, *stp(d, s, h))
        for k in range(0, nz, 8):
            at = pl.ds(k, 8)
            p_east = pr_x[WEST, s, at, :]
            p_ext[pl.ds(k * EXT + LO + bx, 8, stride=EXT), :] = p_east
            p_ext[pl.ds(k * EXT + LO - 1, 8, stride=EXT), :] = pr_x[EAST, s, at, :]
            uh = uh_x[at, :]
            u_ext[pl.ds(k * EXT + LO + bx, 8, stride=EXT), :] = uh
            wet = wet_x[at, :]
            un = wet * (uh - HC * (p_east - ps_x[EAST, s, at, :]))
            uh_x[at, :] = un - relax_hx * (un - wet * ub_x[at, :])
        vn_h = wet_y * (vh - HC * (pltpu.roll(pr_y[SOUTH - 2, s], by - 1, 1) - ps_y[s]))
        vh_next = vn_h - relax_hy * (vn_h - wet_y * vb_y)
        halo = jnp.where(even, vn_h, pltpu.roll(pr_y[NORTH - 2, s], 1, 1))

        def down(kc, carry):
            q_prev, d_prev = carry
            k0 = kc * CHUNK
            stores = []
            for i in range(CHUNK):
                k = k0 + i
                wet = t0 <= k
                p0 = p_ext[own(k), :]
                pm = p_ext[ext_at(k, LO - 1, bx), :]
                p1 = p_ext[ext_at(k, LO + 1, bx), :]
                un = jnp.where(wet, u_ext[own(k), :] - HC * (p0 - pm), 0.0)
                un1 = jnp.where(t1 <= k, u_ext[ext_at(k, LO + 1, bx), :] - HC * (p1 - p0), 0.0)
                hv = pltpu.roll(halo, by - 1 - 2 * k, 1)
                south = jnp.where(lane == 0, hv, pltpu.roll(p0, 1, 1))
                vn = jnp.where(wet, v_ext[own(k), :] - HC * (p0 - south), 0.0)
                vn1 = jnp.where(lane == by - 1, hv, pltpu.roll(vn, by - 1, 1))
                q = jnp.where(wet, p0 - (g[k] * HC) * ((un1 - un) + (vn1 - vn)), 0.0)
                d_new = (
                    wi[slab(k), :] * (w_buf[slab(k), :] - ZC * (q - q_prev)) - li[slab(k), :] * d_prev
                )
                u_rel = un - relax * (un - jnp.where(wet, prof[0, k], 0.0))
                v_rel = vn - relax * (vn - jnp.where(wet, prof[1, k], 0.0))
                stores.append((k, q, d_new, u_rel, v_rel))
                q_prev, d_prev = q, d_new
            for k, q, d_new, u_rel, v_rel in stores:
                q_buf[slab(k), :] = q
                d_buf[slab(k), :] = d_new
                u_ext[own(k), :] = u_rel
                v_ext[own(k), :] = v_rel
            return q_prev, d_prev

        q_last, d_last = lax.fori_loop(0, nz // CHUNK, down, (zero, zero))
        top = (
            wi[pl.ds(nz * bx, bx), :] * (w_buf[pl.ds(nz * bx, bx), :] + ZC * q_last)
            - li[pl.ds(nz * bx, bx), :] * d_last
        )

        def up(kc, carry):
            x, acc = carry
            k0 = nz - CHUNK - kc * CHUNK
            stores = []
            for i in range(CHUNK - 1, -1, -1):
                k = k0 + i
                below = d_buf[slab(k), :] - cc[slab(k), :] * x
                p = (q_buf[slab(k), :] - (g[k] * ZC) * (x - below)) * keep
                acc = jnp.where((lane >> 1) == k, pltpu.roll(p, (2 * k + 1), 1), acc)
                stores.append((k, p, x * keep))
                x = below
            for k, p, w in stores:
                p_ext[own(k), :] = p
                w_buf[slab(k + 1), :] = w
            return x, acc

        carry = (top, zero)
        for kc in range(nz // CHUNK):
            carry = up(kc, carry)

            @pl.when(s < SUB - 1)
            def _(kc=kc):
                send_x(s + 1, nz // CHUNK - 1 - kc)

        acc = carry[1]

        for d in range(4):
            for h in parts(d):
                wait_send(d, *stp(d, s, h))

        @pl.when(s < SUB - 1)
        def _():
            send_y(s + 1, acc)

        return vh_next

    lax.fori_loop(0, SUB, substep, vh0)

    def finish(k, carry):
        u_out[slab(k), :] = u_ext[own(k), :]
        v_out[slab(k), :] = v_ext[own(k), :]
        w_out[slab(k), :] = w_buf[slab(k + 1), :]
        p_out[slab(k), :] = p_ext[own(k), :]
        return carry

    lax.fori_loop(0, nz, finish, 0, unroll=4)


def solution(mesh):
    cnt = (mesh.shape["gx"], mesh.shape["gy"])

    def on_device(u, v, w, p, terr, zone, g, prof):
        nz, bx, by = u.shape
        assert by == 128 and bx % 8 == 0 and 2 * nz == by
        flat = [a.reshape(nz * bx, by) for a in (u, v, w, p)]
        f32 = jnp.float32
        vm = pltpu.VMEM
        ext = vm((nz * EXT + 8, by), f32)
        lev = vm((nz * bx, by), f32)
        lev1 = vm(((nz + 1) * bx, by), f32)
        strip = nz * 8 * bx // by
        dma = pltpu.SemaphoreType.DMA
        scratch = [
            ext, ext, ext, ext,
            vm((4, nz * bx, by), f32),
            lev, lev1, lev1, lev1, lev1, lev1,
            vm((2, 4, 3 * nz, by), f32),
            vm((2, 4, 3 * nz, by), f32),
            vm((2, 4, strip, by), f32),
            vm((2, 4, strip, by), f32),
            vm((4, strip, by), f32),
            vm((4, strip, by), f32),
            vm((8, by), jnp.int32),
            vm((bx, by), jnp.int32),
            vm((bx + 8, by), jnp.int32),
            vm((2, SUB, nz, by), f32),
            vm((2, SUB, nz, by), f32),
            vm((SUB, bx, by), f32),
            vm((2, SUB, bx, by), f32),
            vm((nz, by), f32),
            vm((nz, by), f32),
            vm((bx, by), f32),
            vm((bx, by), f32),
            vm((nz, by), f32),
            vm((nz, by), f32),
            vm((nz, by), f32),
            dma((4, 4)), dma((4, 4)),
            dma((2,)), dma((2,)),
            dma((2,)), dma((2,)),
            dma((4, SUB, nz // CHUNK)), dma((4, SUB, nz // CHUNK)),
        ]
        vspec = pl.BlockSpec(memory_space=pltpu.VMEM)
        sspec = pl.BlockSpec(memory_space=pltpu.SMEM)
        outs = pl.pallas_call(
            functools.partial(kernel, nz, bx, cnt),
            out_shape=[jax.ShapeDtypeStruct((nz * bx, by), f32)] * 4,
            in_specs=[vspec] * 5 + [sspec] * 3,
            out_specs=[vspec] * 4,
            scratch_shapes=scratch,
            compiler_params=pltpu.CompilerParams(collective_id=0, has_side_effects=True),
        )(*flat, terr, zone, g, prof)
        return tuple(a.reshape(nz, bx, by) for a in outs)

    field = P(None, "gx", "gy")
    return jax.shard_map(
        on_device,
        mesh=mesh,
        in_specs=(field, field, field, field, P("gx", "gy"), P(), P(), P()),
        out_specs=(field,) * 4,
        check_vma=False,
    )
```
